32 devices in a mesh: pts: 8 (over z, core), head: 4 (over y, x).
Axes of the slice: x: 2, y: 2, z: 4, core: 2. Of those that a mesh axis runs over, the one named last changes fastest.
Arguments:
- points: bfloat16 [73728, 128], P('pts')
- counts: int32 [8], P('pts'), may hold values from 1 to 9216, 55296 in all
- ln1_gain: float32 [2, 128], replicated, may hold values from 0.5 to 1.5
- ln1_bias: float32 [2, 128], replicated, may hold values from -1.5 to 1.5
- w_in: bfloat16 [2, 128, 128], P(None, None, 'head'), may hold values from -0.5 to 0.5
- w_fx: bfloat16 [2, 128, 128], P(None, None, 'head'), may hold values from -0.5 to 0.5
- w_slice: bfloat16 [2, 32, 32], replicated
- temper: float32 [2, 4], replicated, may hold values from 0.5 to 2
- query_weight: bfloat16 [2, 32, 32], replicated
- key_weight: bfloat16 [2, 32, 32], replicated, may hold values from -1 to 1
- value_weight: bfloat16 [2, 32, 32], replicated, may hold values from -1 to 1
- w_out: bfloat16 [2, 128, 128], P(None, 'head'), may hold values from -1 to 1
- b_out: float32 [2, 128], replicated, may hold values from -1.5 to 1.5
- ln2_gain: float32 [2, 128], replicated, may hold values from 0.5 to 1.5
- ln2_bias: float32 [2, 128], replicated, may hold values from -1.5 to 1.5
- w_up: bfloat16 [2, 128, 512], replicated, may hold values from -0.5 to 0.5
- w_down: bfloat16 [2, 512, 128], replicated, may hold values from -0.25 to 0.25
Outputs:
- features: bfloat16 [73728, 128], P(('pts', 'head'))
The draws below stay inside these ranges and needn't reach their ends.
Inputs may be any that keep to these rules, and one draw needn't show every extreme that they name: counts[i] live points fill the first slots of shard i; at least one shard is full; they sum to 55296.
All inputs are finite; a program needn't handle non-finite values.
Results may differ from the reference program's by a relative error of at most 0.014.
Values may be sent and summed in bfloat16 or wider, within the bound.
A program may use at most 128 MiB of HBM per device.

```python
import math
import jax
import jax.numpy as jnp
import numpy as np
from jax import lax

DH = 32
H = 4
C = 128
M = 32
FF = 512
LAYERS = 2
P_DEV = 9216
POINTS = 73728
N_PTS = 8


def draw_points(key, part):
    k_base, k_shard, k_region = jax.random.split(jax.random.fold_in(key, 11), 3)
    base = jax.random.normal(k_base, (POINTS, C), jnp.float32)
    shard_shift = jax.random.normal(k_shard, (POINTS // P_DEV, C), jnp.float32) * 1.5
    region_shift = jax.random.normal(k_region, (POINTS // 64, C), jnp.float32) * 0.7
    value = base + jnp.repeat(shard_shift, P_DEV, axis=0) + jnp.repeat(region_shift, 64, axis=0)
    return value.astype(jnp.bfloat16)


def draw_w_slice(key, part):
    k_main = jax.random.fold_in(jax.random.fold_in(key, 23), 0)
    value = jax.random.normal(k_main, (LAYERS, DH, M), jnp.float32) * (3.0 / math.sqrt(DH))
    return value.astype(jnp.bfloat16)


def draw_query_weight(key, part):
    k_main = jax.random.fold_in(jax.random.fold_in(key, 37), 0)
    value = jax.random.normal(k_main, (LAYERS, DH, DH), jnp.float32) / math.sqrt(DH)
    return value.astype(jnp.bfloat16)


def block_scale(own_key, dims, cuts, low, high):
    loudness = 1.0
    for position, parts in cuts:
        draws = jax.random.uniform(jax.random.fold_in(jax.random.fold_in(own_key, 6), position), (parts,), jnp.float32, low / len(cuts), high / len(cuts))
        loudness = loudness * jnp.repeat(jnp.exp(draws), dims[position] // parts).reshape((-1,) + (1,) * (len(dims) - 1 - position))
    return loudness


def profile(number_of, total, reach, lean):
    weights = [(1 << 20) // math.isqrt(rank ** lean) + 1 for rank in range(2, number_of + 1)]
    surplus, holding = total - reach - (number_of - 1), [1] * (number_of - 1)
    while surplus > 0:
        free = [i for i in range(number_of - 1) if holding[i] < reach]
        mass, budget = sum([weights[i] for i in free]), surplus
        for i in free:
            more = min(reach - holding[i], max(1, budget * weights[i] // mass), surplus)
            holding[i] = holding[i] + more
            surplus = surplus - more
    return np.array([reach] + holding)


def uneven(stream_key, count, total, bound, skew):
    if count == 2:
        one = jax.random.randint(stream_key, (), max(1, total - bound), min(bound, total - 1) + 1)
        return jnp.stack([one, total - one])
    tallies = jnp.asarray(profile(count, total, bound, skew), jnp.int32)
    pairs = (count - 1) // 2
    source_of, taker = tallies[1:1 + 2 * pairs:2], tallies[2:2 + 2 * pairs:2]
    room = jnp.minimum(source_of - 1, bound - taker)
    moved = jax.random.randint(jax.random.fold_in(stream_key, 1), (pairs,), 0, 1 << 20) % (room + 1)
    tallies = tallies.at[1:1 + 2 * pairs:2].set(source_of - moved).at[2:2 + 2 * pairs:2].set(taker + moved)
    return tallies[jax.random.permutation(jax.random.fold_in(stream_key, 2), count)]


def noise(own_key, dims, scale, limit, pieces=(), held_as=jnp.bfloat16):
    array = scale * jax.random.normal(own_key, dims, jnp.float32)
    if pieces:
        array = array * block_scale(own_key, dims, pieces, -0.22, 0.18)
    return jnp.clip(array, -limit, limit).astype(held_as)


def setup_inputs(seed: int = 0) -> dict:
    seeds = jax.random.split(jax.random.key(seed), 18)
    points = draw_points(jax.random.fold_in(seeds[17], 71), 0)
    counts = uneven(seeds[1], N_PTS, 3 * POINTS // 4, P_DEV, 1).astype(jnp.int32)
    ln1_gain = jnp.clip(1.0 + 0.1 * jax.random.normal(seeds[2], (LAYERS, C), jnp.float32), 0.5, 1.5)
    ln1_bias = noise(seeds[3], (LAYERS, C), 0.3, 1.5, (), jnp.float32)
    w_in = noise(seeds[4], (LAYERS, C, C), C ** -0.5, 0.5, ((2, 4),))
    w_fx = noise(seeds[5], (LAYERS, C, C), C ** -0.5, 0.5, ((2, 4),))
    w_slice = draw_w_slice(jax.random.fold_in(seeds[17], 71), 0)
    temper = jnp.clip(jnp.exp(jax.random.uniform(seeds[7], (LAYERS, H), jnp.float32, math.log(0.5), math.log(2.0))), 0.5, 2.0)
    query_weight = draw_query_weight(jax.random.fold_in(seeds[17], 71), 0)
    key_weight = noise(seeds[9], (LAYERS, DH, DH), DH ** -0.5, 1.0)
    value_weight = noise(seeds[10], (LAYERS, DH, DH), DH ** -0.5, 1.0)
    w_out = noise(seeds[11], (LAYERS, C, C), DH ** -0.5, 1.0, ((1, 4),))
    b_out = noise(seeds[12], (LAYERS, C), 0.3, 1.5, (), jnp.float32)
    ln2_gain = jnp.clip(1.0 + 0.1 * jax.random.normal(seeds[13], (LAYERS, C), jnp.float32), 0.5, 1.5)
    ln2_bias = noise(seeds[14], (LAYERS, C), 0.3, 1.5, (), jnp.float32)
    w_up = noise(seeds[15], (LAYERS, C, FF), C ** -0.5, 0.5)
    w_down = noise(seeds[16], (LAYERS, FF, C), FF ** -0.5, 0.25)
    return dict(points=points, counts=counts, ln1_gain=ln1_gain, ln1_bias=ln1_bias, w_in=w_in, w_fx=w_fx, w_slice=w_slice, temper=temper, query_weight=query_weight, key_weight=key_weight, value_weight=value_weight, w_out=w_out, b_out=b_out, ln2_gain=ln2_gain, ln2_bias=ln2_bias, w_up=w_up, w_down=w_down)


def layer_norm(value, gain, bias):
    mean = lax.optimization_barrier(jnp.mean(value, axis=-1, keepdims=True))
    centred = value - mean
    var = lax.optimization_barrier(jnp.mean(centred * centred, axis=-1, keepdims=True))
    return centred * lax.rsqrt(var + 1e-05) * gain + bias

def reference(points, counts, ln1_gain, ln1_bias, w_in, w_fx, w_slice, temper, query_weight, key_weight, value_weight, w_out, b_out, ln2_gain, ln2_bias, w_up, w_down):
    total_rows = points.shape[0]
    index = jnp.arange(total_rows, dtype=jnp.int32)
    shard_count = jnp.take(counts, index // P_DEV)
    live = (index % P_DEV < shard_count).astype(jnp.float32)
    head_parts = lax.Precision.HIGHEST
    state = points
    for layer_index in range(LAYERS):
        normed = layer_norm(state.astype(jnp.float32), ln1_gain[layer_index], ln1_bias[layer_index]).astype(jnp.bfloat16)
        mid = jnp.dot(normed, w_in[layer_index], preferred_element_type=jnp.float32).astype(jnp.bfloat16)
        feats = jnp.dot(normed, w_fx[layer_index], preferred_element_type=jnp.float32).astype(jnp.bfloat16)
        logits = jnp.dot(mid.reshape(total_rows * H, DH), w_slice[layer_index], preferred_element_type=jnp.float32)
        logits = logits.reshape(total_rows, H, M) / temper[layer_index][None, :, None]
        weights = jax.nn.softmax(logits, axis=-1) * live[:, None, None]
        half_weights = weights.astype(jnp.bfloat16)
        features_three = feats.reshape(total_rows, H, DH).astype(jnp.float32)
        numerator = jnp.einsum('oqw,oqs->qws', half_weights.astype(jnp.float32), features_three, precision=head_parts)
        total = lax.optimization_barrier(jnp.sum(weights, axis=0))
        token_rows = numerator / jnp.maximum(total, 1.0)[..., None]
        query_rows = jnp.einsum('aur,rz->auz', token_rows, query_weight[layer_index].astype(jnp.float32), precision=head_parts)
        slice_keys = jnp.einsum('aur,rz->auz', token_rows, key_weight[layer_index].astype(jnp.float32), precision=head_parts)
        slice_values = jnp.einsum('aur,rz->auz', token_rows, value_weight[layer_index].astype(jnp.float32), precision=head_parts)
        scores = jnp.einsum('hme,hke->hmk', query_rows, slice_keys, precision=head_parts) * DH ** (-0.5)
        attn = jax.nn.softmax(scores, axis=-1)
        mixed_token = jnp.einsum('hmk,hke->hme', attn, slice_values, precision=head_parts).astype(jnp.bfloat16)
        unslice_tokens = jnp.einsum('roe,oew->row', half_weights.astype(jnp.float32), mixed_token.astype(jnp.float32), precision=head_parts)
        unslice_tokens = unslice_tokens.astype(jnp.bfloat16).reshape(total_rows, H * DH)
        after = state.astype(jnp.float32) + jnp.dot(unslice_tokens, w_out[layer_index], preferred_element_type=jnp.float32) + b_out[layer_index]
        normed2 = layer_norm(after, ln2_gain[layer_index], ln2_bias[layer_index]).astype(jnp.bfloat16)
        upper = jax.nn.gelu(jnp.dot(normed2, w_up[layer_index], preferred_element_type=jnp.float32)).astype(jnp.bfloat16)
        state = (after + jnp.dot(upper, w_down[layer_index], preferred_element_type=jnp.float32)).astype(jnp.bfloat16)
    return state
```

```python
import jax
import jax.numpy as jnp
from jax import lax
from jax.sharding import PartitionSpec as P

DH = 32
M = 32


def layer_norm(value, gain, bias):
    mean = jnp.mean(value, axis=-1, keepdims=True)
    centred = value - mean
    var = jnp.mean(centred * centred, axis=-1, keepdims=True)
    return centred * lax.rsqrt(var + 1e-05) * gain + bias


def slice_attention(token_rows, query_weight, key_weight, value_weight):
    head_parts = lax.Precision.HIGHEST
    query_rows = jnp.einsum(
        "aur,rz->auz", token_rows, query_weight.astype(jnp.float32), precision=head_parts
    )
    slice_keys = jnp.einsum(
        "aur,rz->auz", token_rows, key_weight.astype(jnp.float32), precision=head_parts
    )
    slice_values = jnp.einsum(
        "aur,rz->auz", token_rows, value_weight.astype(jnp.float32), precision=head_parts
    )
    scores = jnp.einsum("hme,hke->hmk", query_rows, slice_keys, precision=head_parts) * DH ** (-0.5)
    attn = jax.nn.softmax(scores, axis=-1)
    return jnp.einsum("hmk,hke->hme", attn, slice_values, precision=head_parts).astype(jnp.bfloat16)


def body(
    points,
    counts,
    ln1_gain,
    ln1_bias,
    w_in,
    w_fx,
    w_slice,
    temper,
    query_weight,
    key_weight,
    value_weight,
    w_out,
    b_out,
    ln2_gain,
    ln2_bias,
    w_up,
    w_down,
):
    groups = lax.axis_size("head")
    rows = points.shape[0] // groups
    first_row = lax.axis_index("head") * rows
    layers = w_in.shape[0]
    full_in = lax.all_gather(w_in, "head", axis=2, tiled=True)
    full_fx = lax.all_gather(w_fx, "head", axis=2, tiled=True)
    full_out = lax.all_gather(w_out, "head", axis=1, tiled=True)
    heads = full_in.shape[2] // DH
    live = (first_row + jnp.arange(rows, dtype=jnp.int32) < counts[0]).astype(jnp.float32)
    current = lax.dynamic_slice_in_dim(points, first_row, rows, 0)
    for layer_index in range(layers):
        normed = layer_norm(
            current.astype(jnp.float32), ln1_gain[layer_index], ln1_bias[layer_index]
        ).astype(jnp.bfloat16)
        mid = jnp.dot(normed, full_in[layer_index], preferred_element_type=jnp.float32).astype(
            jnp.bfloat16
        )
        feats = jnp.dot(normed, full_fx[layer_index], preferred_element_type=jnp.float32).astype(
            jnp.bfloat16
        )
        spread = jnp.kron(jnp.eye(heads, dtype=jnp.bfloat16), w_slice[layer_index])
        logits = jnp.dot(mid, spread, preferred_element_type=jnp.float32)
        logits = logits.reshape(rows, heads, M) / temper[layer_index][None, :, None]
        weights = jax.nn.softmax(logits, axis=-1) * live[:, None, None]
        half_weights = weights.astype(jnp.bfloat16).reshape(rows, heads * M)
        total = jnp.sum(weights, axis=0)
        square = jnp.einsum("rs,rl->sl", half_weights, feats, preferred_element_type=jnp.float32)
        square = square.reshape(heads, M, heads, DH)
        numerator = jnp.stack([square[h, :, h, :] for h in range(heads)])
        numerator, total = lax.psum((numerator, total), ("pts", "head"))
        token_rows = numerator / jnp.maximum(total, 1.0)[..., None]
        mixed_token = slice_attention(
            token_rows,
            query_weight[layer_index],
            key_weight[layer_index],
            value_weight[layer_index],
        )
        wide = jnp.einsum(
            "hmv,hvc->hmc",
            mixed_token,
            full_out[layer_index].reshape(heads, DH, -1),
            preferred_element_type=jnp.float32,
        ).astype(jnp.bfloat16).reshape(heads * M, -1)
        projected = jnp.dot(half_weights, wide, preferred_element_type=jnp.float32)
        after = current.astype(jnp.float32) + projected + b_out[layer_index]
        normed2 = layer_norm(after, ln2_gain[layer_index], ln2_bias[layer_index]).astype(
            jnp.bfloat16
        )
        upper = jax.nn.gelu(
            jnp.dot(normed2, w_up[layer_index], preferred_element_type=jnp.float32)
        ).astype(jnp.bfloat16)
        current = (
            after + jnp.dot(upper, w_down[layer_index], preferred_element_type=jnp.float32)
        ).astype(jnp.bfloat16)
    return current


def solution(mesh):
    placed = (
        P("pts", None),
        P("pts"),
        P(),
        P(),
        P(None, None, "head"),
        P(None, None, "head"),
        P(),
        P(),
        P(),
        P(),
        P(),
        P(None, "head", None),
        P(),
        P(),
        P(),
        P(),
        P(),
    )
    return jax.shard_map(
        body, mesh=mesh, in_specs=placed, out_specs=P(("pts", "head"), None), check_vma=False
    )
```

```python
import functools
import math

import jax
import jax.numpy as jnp
from jax import lax
from jax.experimental import pallas as pl
from jax.experimental.pallas import tpu as pltpu
from jax.sharding import PartitionSpec as P

DH = 32
M = 32
TILE = 768
MESH = pl.DeviceIdType.MESH
HIGH = lax.Precision.HIGHEST
F32 = jnp.float32
BF16 = jnp.bfloat16
NT = (((1,), (1,)), ((), ()))


def norm_columns(value, gain, bias):
    mean = jnp.mean(value, axis=0, keepdims=True)
    centred = value - mean
    var = jnp.mean(centred * centred, axis=0, keepdims=True)
    return centred * lax.rsqrt(var + 1e-05) * gain + bias


def kernel(
    groups,
    shards,
    rows,
    tiles,
    counts,
    temper,
    points,
    ln1_gain,
    ln1_bias,
    w_in,
    w_fx,
    w_slice,
    query_weight,
    key_weight,
    value_weight,
    w_out,
    b_out,
    ln2_gain,
    ln2_bias,
    w_up,
    w_down,
    out,
    x_rows,
    x_cols,
    normed_ref,
    weights_ref,
    wl_ref,
    up_t,
    down_t,
    fx_pad,
    par,
    par_cols,
    sums,
    recv_a,
    own_b,
    recv_b,
    g_ref,
    row_sem,
    wl_send,
    wl_recv,
    a_send,
    a_recv,
    b_send,
    b_recv,
    c_send,
    c_recv,
):
    layers, _, width = w_in.shape
    spread = groups * M
    hd = lax.axis_index("head")
    pt = lax.axis_index("pts")

    def head_peer(k):
        return lax.rem(hd + k, groups)

    def pts_peer(k):
        return lax.rem(pt + k, shards)

    barrier = pltpu.get_barrier_semaphore()
    for k in range(1, groups):
        pl.semaphore_signal(barrier, inc=1, device_id={"head": head_peer(k)}, device_id_type=MESH)
    for k in range(1, shards):
        pl.semaphore_signal(barrier, inc=1, device_id={"pts": pts_peer(k)}, device_id_type=MESH)
    first = pl.multiple_of(hd * rows, 64)
    load = pltpu.make_async_copy(
        points.at[pl.ds(first, rows)], x_rows.at[pl.ds(0, rows)], row_sem
    )
    load.start()

    own_head = pl.ds(pl.multiple_of(hd * M, M), M)
    for l in range(layers):
        scale = jnp.full((M, width), temper[l, hd], F32)
        w_head = w_in[l].astype(F32)
        slicer = w_slice[l].astype(F32).T
        folded = jnp.dot(slicer, w_head, preferred_element_type=F32, precision=HIGH)
        wl_ref[l, own_head, :] = (folded * math.log2(math.e) / scale).astype(BF16)
    pl.semaphore_wait(barrier, groups + shards - 2)

    wl_copies = []
    for k in range(1, groups):
        for l in range(layers):
            copy = pltpu.make_async_remote_copy(
                src_ref=wl_ref.at[l, own_head],
                dst_ref=wl_ref.at[l, own_head],
                send_sem=wl_send.at[l, k],
                recv_sem=wl_recv.at[l, k],
                device_id={"head": head_peer(k)},
                device_id_type=MESH,
            )
            copy.start()
            wl_copies.append(copy)

    par[...] = jnp.zeros_like(par)
    for i, ref in enumerate((ln1_gain, ln1_bias, b_out, ln2_gain, ln2_bias)):
        par[i * layers : (i + 1) * layers, :] = ref[...]
    par_t = par[...].T
    for i in range(5 * layers):
        par_cols[i] = jnp.broadcast_to(par_t[:, i : i + 1], (width, TILE))
    fx_pad[...] = jnp.zeros_like(fx_pad)
    for l in range(layers):
        fx_pad[l, :DH, :] = w_fx[l].astype(F32)
    if tiles * TILE > rows:
        x_rows[rows:, :] = jnp.zeros((tiles * TILE - rows, width), BF16)
    load.wait()

    def param(i, l):
        return par_cols[i * layers + l]

    def first_half(l, t, normed):
        logits = jnp.dot(wl_ref[l], normed, preferred_element_type=F32)
        logits = logits.reshape(groups, M, TILE)
        top = jnp.max(logits, axis=1, keepdims=True)
        grown = jnp.exp2(logits - top)
        index = t * TILE + lax.broadcasted_iota(jnp.int32, (1, 1, TILE), 2)
        live = jnp.logical_and(index < rows, index + hd * rows < counts[0]).astype(F32)
        weights = grown * (live / jnp.sum(grown, axis=1, keepdims=True))
        half = weights.reshape(spread, TILE).astype(BF16)
        weights_ref[t] = half
        both = jnp.concatenate([normed, jnp.ones((128, TILE), BF16)], axis=0)
        sums[l] += lax.dot_general(half, both, NT, preferred_element_type=F32)

    def second_half(l, t, g_t):
        x = x_cols[t].astype(F32)
        after = x + jnp.dot(g_t, weights_ref[t], preferred_element_type=F32) + param(2, l)
        normed = norm_columns(after, param(3, l), param(4, l)).astype(BF16)
        upper = jnp.dot(up_t[l], normed, preferred_element_type=F32)
        inner = upper * (0.7978845608028654 + 0.035677408136300125 * (upper * upper))
        half = 0.5 * upper
        upper = (half + half * jnp.tanh(inner)).astype(BF16)
        return (after + jnp.dot(down_t[l], upper, preferred_element_type=F32)).astype(BF16)

    def exchange(l):
        copies = []
        for k in range(1, groups):
            copy = pltpu.make_async_remote_copy(
                src_ref=sums.at[l, pl.ds(pl.multiple_of(head_peer(k) * M, M), M)],
                dst_ref=recv_a.at[l, k],
                send_sem=a_send.at[l, k],
                recv_sem=a_recv.at[l, k],
                device_id={"head": head_peer(k)},
                device_id_type=MESH,
            )
            copy.start()
            copies.append(copy)
        up_t[l] = w_up[l].astype(F32).T.astype(BF16)
        down_t[l] = w_down[l].astype(F32).T.astype(BF16)
        for copy in copies:
            copy.wait()
        square = sums[l, own_head, :]
        for k in range(1, groups):
            square = square + recv_a[l, k]
        numer = lax.dot_general(
            square[:, :width], fx_pad[l], NT, preferred_element_type=F32, precision=HIGH
        )
        lane = lax.broadcasted_iota(jnp.int32, (M, 128), 1)
        own_b[l] = jnp.where(lane < DH, numer, square[:, width:])
        copies = []
        for k in range(1, shards):
            copy = pltpu.make_async_remote_copy(
                src_ref=own_b.at[l],
                dst_ref=recv_b.at[l, k],
                send_sem=b_send.at[l, k],
                recv_sem=b_recv.at[l, k],
                device_id={"pts": pts_peer(k)},
                device_id_type=MESH,
            )
            copy.start()
            copies.append(copy)
        for copy in copies:
            copy.wait()
        summed = own_b[l]
        for k in range(1, shards):
            summed = summed + recv_b[l, k]
        token = summed[:, :DH] / jnp.maximum(summed[:, 127:128], 1.0)
        query = jnp.dot(token, query_weight[l].astype(F32), preferred_element_type=F32, precision=HIGH)
        keys = jnp.dot(token, key_weight[l].astype(F32), preferred_element_type=F32, precision=HIGH)
        value = jnp.dot(token, value_weight[l].astype(F32), preferred_element_type=F32, precision=HIGH)
        scores = lax.dot_general(query, keys, NT, preferred_element_type=F32, precision=HIGH)
        attn = jax.nn.softmax(scores * DH ** (-0.5), axis=-1)
        mixed = jnp.dot(attn, value, preferred_element_type=F32, precision=HIGH).astype(BF16)
        wide = jnp.dot(mixed, w_out[l], preferred_element_type=F32)
        g_ref[l, own_head, :] = wide.astype(BF16)
        copies = []
        for k in range(1, groups):
            copy = pltpu.make_async_remote_copy(
                src_ref=g_ref.at[l, own_head],
                dst_ref=g_ref.at[l, own_head],
                send_sem=c_send.at[l, k],
                recv_sem=c_recv.at[l, k],
                device_id={"head": head_peer(k)},
                device_id_type=MESH,
            )
            copy.start()
            copies.append(copy)
        for copy in copies:
            copy.wait()
        return g_ref[l].astype(F32).T.astype(BF16)

    sums[...] = jnp.zeros_like(sums)

    @pl.loop(0, tiles)
    def _(t):
        at = pl.ds(pl.multiple_of(t * TILE, TILE), TILE)
        x = x_rows[at, :].astype(F32).T
        x_cols[t] = x.astype(BF16)
        normed_ref[t] = norm_columns(x, param(0, 0), param(1, 0)).astype(BF16)

    for copy in wl_copies:
        copy.wait()

    @pl.loop(0, tiles)
    def _(t):
        first_half(0, t, normed_ref[t])

    for l in range(layers):
        g_t = exchange(l)

        @pl.loop(0, tiles)
        def _(t, l=l, g_t=g_t):
            x = second_half(l, t, g_t)
            if l < layers - 1:
                x_cols[t] = x
                normed = norm_columns(x.astype(F32), param(0, l + 1), param(1, l + 1))
                first_half(l + 1, t, normed.astype(BF16))
            else:
                at = pl.ds(pl.multiple_of(t * TILE, TILE), TILE)
                x_rows[at, :] = x.astype(F32).T.astype(BF16)

    store = pltpu.make_async_copy(x_rows.at[pl.ds(0, rows)], out, row_sem)
    store.start()
    store.wait()


def body(
    points,
    counts,
    ln1_gain,
    ln1_bias,
    w_in,
    w_fx,
    w_slice,
    temper,
    query_weight,
    key_weight,
    value_weight,
    w_out,
    b_out,
    ln2_gain,
    ln2_bias,
    w_up,
    w_down,
):
    groups = lax.axis_size("head")
    shards = lax.axis_size("pts")
    rows = points.shape[0] // groups
    layers, width, part = w_in.shape
    assert part == DH
    hidden = w_up.shape[2]
    spread = groups * M
    tiles = -(-rows // TILE)
    vmem = pl.BlockSpec(memory_space=pltpu.VMEM)
    smem = pl.BlockSpec(memory_space=pltpu.SMEM)
    hbm = pl.BlockSpec(memory_space=pl.ANY)
    dma = pltpu.SemaphoreType.DMA
    return pl.pallas_call(
        functools.partial(kernel, groups, shards, rows, tiles),
        out_shape=jax.ShapeDtypeStruct((rows, width), BF16),
        in_specs=[smem, smem, hbm] + [vmem] * 14,
        out_specs=hbm,
        scratch_shapes=[
            pltpu.VMEM((tiles * TILE, width), BF16),
            pltpu.VMEM((tiles, width, TILE), BF16),
            pltpu.VMEM((tiles, width, TILE), BF16),
            pltpu.VMEM((tiles, spread, TILE), BF16),
            pltpu.VMEM((layers, spread, width), BF16),
            pltpu.VMEM((layers, hidden, width), BF16),
            pltpu.VMEM((layers, width, hidden), BF16),
            pltpu.VMEM((layers, 128, width), F32),
            pltpu.VMEM((-(-5 * layers // 8) * 8, width), F32),
            pltpu.VMEM((5 * layers, width, TILE), F32),
            pltpu.VMEM((layers, spread, width + 128), F32),
            pltpu.VMEM((layers, groups, M, width + 128), F32),
            pltpu.VMEM((layers, M, 128), F32),
            pltpu.VMEM((layers, shards, M, 128), F32),
            pltpu.VMEM((layers, spread, width), BF16),
            dma,
            dma((layers, groups)),
            dma((layers, groups)),
            dma((layers, groups)),
            dma((layers, groups)),
            dma((layers, shards)),
            dma((layers, shards)),
            dma((layers, groups)),
            dma((layers, groups)),
        ],
        compiler_params=pltpu.CompilerParams(collective_id=0, has_side_effects=True),
    )(
        counts,
        temper,
        points,
        ln1_gain,
        ln1_bias,
        w_in.swapaxes(1, 2),
        w_fx.swapaxes(1, 2),
        w_slice,
        query_weight,
        key_weight,
        value_weight,
        w_out,
        b_out,
        ln2_gain,
        ln2_bias,
        w_up,
        w_down,
    )


def solution(mesh):
    placed = (
        P("pts", None),
        P("pts"),
        P(),
        P(),
        P(None, None, "head"),
        P(None, None, "head"),
        P(),
        P(),
        P(),
        P(),
        P(),
        P(None, "head", None),
        P(),
        P(),
        P(),
        P(),
        P(),
    )
    return jax.shard_map(
        body, mesh=mesh, in_specs=placed, out_specs=P(("pts", "head"), None), check_vma=False
    )
```

```python
import functools
import math

import jax
import jax.numpy as jnp
from jax import lax
from jax.experimental import pallas as pl
from jax.experimental.pallas import tpu as pltpu
from jax.sharding import PartitionSpec as P

DH = 32
M = 32
TILE = 768
MESH = pl.DeviceIdType.MESH
HIGH = lax.Precision.HIGHEST
F32 = jnp.float32
BF16 = jnp.bfloat16
NT = (((1,), (1,)), ((), ()))


def norm_columns(value, gain, bias):
    mean = jnp.mean(value, axis=0, keepdims=True)
    centred = value - mean
    var = jnp.mean(centred * centred, axis=0, keepdims=True)
    return centred * lax.rsqrt(var + 1e-05) * gain + bias


def kernel(
    groups,
    shards,
    rows,
    tiles,
    counts,
    temper,
    points,
    ln1_gain,
    ln1_bias,
    w_in,
    w_fx,
    w_slice,
    query_weight,
    key_weight,
    value_weight,
    w_out,
    b_out,
    ln2_gain,
    ln2_bias,
    w_up,
    w_down,
    out,
    x_rows,
    x_cols,
    normed_ref,
    weights_ref,
    wl_ref,
    up_t,
    down_t,
    fx_all,
    out_all,
    par,
    par_cols,
    sums,
    pay,
    recv_a,
    own_b,
    recv_b,
    joined,
    maps,
    row_sem,
    wl_send,
    wl_recv,
    a_send,
    a_recv,
    b_send,
    b_recv,
    c_send,
    c_recv,
):
    layers, _, width = w_in.shape
    spread = groups * M
    hd = lax.axis_index("head")
    pt = lax.axis_index("pts")

    def head_peer(k):
        return lax.rem(hd + k, groups)

    def pts_peer(k):
        return lax.rem(pt + k, shards)

    half_m = M // 2
    core = lax.rem(pt, 2)
    near = [(k, j) for k in range(groups) for j in range(2) if k or j]

    def near_id(k, j):
        return {"head": head_peer(k), "pts": pt - core + lax.rem(core + j, 2)}

    barrier = pltpu.get_barrier_semaphore()
    for k, j in near:
        pl.semaphore_signal(barrier, inc=1, device_id=near_id(k, j), device_id_type=MESH)
    for k in range(1, shards):
        pl.semaphore_signal(barrier, inc=1, device_id={"pts": pts_peer(k)}, device_id_type=MESH)
    first = pl.multiple_of(hd * rows, 64)
    load = pltpu.make_async_copy(
        points.at[pl.ds(first, rows)], x_rows.at[pl.ds(0, rows)], row_sem
    )
    load.start()

    own_head = pl.ds(pl.multiple_of(hd * M, M), M)
    for l in range(layers):
        scale = jnp.full((M, width), temper[l, hd], F32)
        w_head = w_in[l].astype(F32)
        slicer = w_slice[l].astype(F32).T
        folded = jnp.dot(slicer, w_head, preferred_element_type=F32, precision=HIGH)
        wl_ref[l, own_head, :] = (folded * math.log2(math.e) / scale).astype(BF16)
    pl.semaphore_wait(barrier, 2 * groups + shards - 2)

    wl_copies = []
    for k in range(1, groups):
        for l in range(layers):
            copy = pltpu.make_async_remote_copy(
                src_ref=wl_ref.at[l, own_head],
                dst_ref=wl_ref.at[l, own_head],
                send_sem=wl_send.at[l, k],
                recv_sem=wl_recv.at[l, k],
                device_id={"head": head_peer(k)},
                device_id_type=MESH,
            )
            copy.start()
            wl_copies.append(copy)
        for i, (mine, everyone) in enumerate(((w_fx, fx_all), (w_out, out_all))):
            copy = pltpu.make_async_remote_copy(
                src_ref=mine,
                dst_ref=everyone.at[:, own_head],
                send_sem=c_send.at[i, k],
                recv_sem=c_recv.at[i, k],
                device_id={"head": head_peer(k)},
                device_id_type=MESH,
            )
            copy.start()
            wl_copies.append(copy)
    fx_all[:, own_head, :] = w_fx[...]
    out_all[:, own_head, :] = w_out[...]

    par[...] = jnp.zeros_like(par)
    for i, ref in enumerate((ln1_gain, ln1_bias, b_out, ln2_gain, ln2_bias)):
        par[i * layers : (i + 1) * layers, :] = ref[...]
    par_t = par[...].T
    for i in range(5 * layers):
        par_cols[i] = jnp.broadcast_to(par_t[:, i : i + 1], (width, TILE))
    if tiles * TILE > rows:
        x_rows[rows:, :] = jnp.zeros((tiles * TILE - rows, width), BF16)
    load.wait()

    def param(i, l):
        return par_cols[i * layers + l]

    def first_half(l, t, normed):
        logits = jnp.dot(wl_ref[l], normed, preferred_element_type=F32)
        logits = logits.reshape(groups, M, TILE)
        top = jnp.max(logits, axis=1, keepdims=True)
        grown = jnp.exp2(logits - top)
        index = t * TILE + lax.broadcasted_iota(jnp.int32, (1, 1, TILE), 2)
        live = jnp.logical_and(index < rows, index + hd * rows < counts[0]).astype(F32)
        weights = grown * (live / jnp.sum(grown, axis=1, keepdims=True))
        half = weights.reshape(spread, TILE).astype(BF16)
        weights_ref[t] = half
        both = jnp.concatenate([normed, jnp.ones((128, TILE), BF16)], axis=0)
        sums[l] += lax.dot_general(half, both, NT, preferred_element_type=F32)

    def second_half(l, t, g_t):
        x = x_cols[t].astype(F32)
        after = x + jnp.dot(g_t, weights_ref[t], preferred_element_type=F32) + param(2, l)
        normed = norm_columns(after, param(3, l), param(4, l)).astype(BF16)
        upper = jnp.dot(up_t[l], normed, preferred_element_type=F32)
        inner = upper * (0.7978845608028654 + 0.035677408136300125 * (upper * upper))
        half = 0.5 * upper
        upper = (half + half * jnp.tanh(inner)).astype(BF16)
        return (after + jnp.dot(down_t[l], upper, preferred_element_type=F32)).astype(BF16)

    def exchange(l):
        heads_of_lane = lax.broadcasted_iota(jnp.int32, (M, spread), 1) >> 5
        square = lax.dot_general(
            sums[l, :, :width],
            fx_all[l].astype(F32),
            NT,
            preferred_element_type=F32,
            precision=HIGH,
        )
        numer = jnp.zeros((M, spread), F32)
        total = jnp.zeros((M, spread), F32)
        for h in range(groups):
            here = heads_of_lane == h
            block = slice(h * M, (h + 1) * M)
            numer = jnp.where(here, square[block], numer)
            total = jnp.where(here, sums[l, block, width : width + 1], total)
        for c in range(2):
            cut = slice(c * half_m, (c + 1) * half_m)
            pay[l, c, :half_m, :] = numer[cut].astype(BF16)
            pay[l, c, half_m:, :] = total[cut].astype(BF16)
        copies = []
        for k, j in near:
            target = lax.rem(core + j, 2)
            copy = pltpu.make_async_remote_copy(
                src_ref=pay.at[l, target],
                dst_ref=recv_a.at[l, 2 * k + j],
                send_sem=a_send.at[l, 2 * k + j],
                recv_sem=a_recv.at[l, 2 * k + j],
                device_id=near_id(k, j),
                device_id_type=MESH,
            )
            copy.start()
            copies.append(copy)
        up_t[l] = w_up[l].astype(F32).T.astype(BF16)
        down_t[l] = w_down[l].astype(F32).T.astype(BF16)
        same_head = (lax.broadcasted_iota(jnp.int32, (spread, spread), 0) >> 5) == (
            lax.broadcasted_iota(jnp.int32, (spread, spread), 1) >> 5
        )
        across = (
            (lax.broadcasted_iota(jnp.int32, (DH, spread), 1) & (DH - 1))
            == lax.broadcasted_iota(jnp.int32, (DH, spread), 0)
        ).astype(F32).astype(BF16)
        down = (
            (lax.broadcasted_iota(jnp.int32, (spread, DH), 0) & (DH - 1))
            == lax.broadcasted_iota(jnp.int32, (spread, DH), 1)
        ).astype(F32).astype(BF16)
        for i, ref in enumerate((query_weight, key_weight, value_weight)):
            wide = jnp.dot(ref[l], across, preferred_element_type=F32).astype(BF16)
            full = jnp.dot(down, wide, preferred_element_type=F32)
            maps[i] = jnp.where(same_head, full, 0.0)
        for copy in copies:
            copy.wait()
        chip = pay[l, core].astype(F32)
        for k, j in near:
            chip = chip + recv_a[l, 2 * k + j].astype(F32)
        own_b[l] = chip.astype(BF16)
        copies = []
        for k in range(1, shards):
            copy = pltpu.make_async_remote_copy(
                src_ref=own_b.at[l],
                dst_ref=recv_b.at[l, k],
                send_sem=b_send.at[l, k],
                recv_sem=b_recv.at[l, k],
                device_id={"pts": pts_peer(k)},
                device_id_type=MESH,
            )
            copy.start()
            copies.append(copy)
        for copy in copies:
            copy.wait()
        halves = [own_b[l].astype(F32), recv_b[l, 1].astype(F32)]
        for k in range(2, shards):
            halves[k % 2] = halves[k % 2] + recv_b[l, k].astype(F32)
        for j in range(2):
            at = pl.ds(pl.multiple_of(lax.rem(core + j, 2) * half_m, half_m), half_m)
            joined[0, at, :] = halves[j][:half_m]
            joined[1, at, :] = halves[j][half_m:]
        token = joined[0] / jnp.maximum(joined[1], 1.0)
        query = jnp.dot(token, maps[0], preferred_element_type=F32, precision=HIGH)
        keys = jnp.dot(token, maps[1], preferred_element_type=F32, precision=HIGH)
        value = jnp.dot(token, maps[2], preferred_element_type=F32, precision=HIGH)
        query = jnp.where(same_head, jnp.concatenate([query] * groups, axis=0), 0.0)
        scores = lax.dot_general(query, keys, NT, preferred_element_type=F32, precision=HIGH)
        attn = jax.nn.softmax(scores * DH ** (-0.5), axis=-1)
        mixed = jnp.dot(attn, value, preferred_element_type=F32, precision=HIGH)
        mixed = jnp.where(same_head, mixed, 0.0).astype(BF16)
        return jnp.dot(mixed, out_all[l], preferred_element_type=F32).T.astype(BF16)

    sums[...] = jnp.zeros_like(sums)

    @pl.loop(0, tiles)
    def _(t):
        at = pl.ds(pl.multiple_of(t * TILE, TILE), TILE)
        x = x_rows[at, :].astype(F32).T
        x_cols[t] = x.astype(BF16)
        normed_ref[t] = norm_columns(x, param(0, 0), param(1, 0)).astype(BF16)

    for copy in wl_copies:
        copy.wait()

    @pl.loop(0, tiles)
    def _(t):
        first_half(0, t, normed_ref[t])

    for l in range(layers):
        g_t = exchange(l)

        @pl.loop(0, tiles)
        def _(t, l=l, g_t=g_t):
            x = second_half(l, t, g_t)
            if l < layers - 1:
                x_cols[t] = x
                normed = norm_columns(x.astype(F32), param(0, l + 1), param(1, l + 1))
                first_half(l + 1, t, normed.astype(BF16))
            else:
                at = pl.ds(pl.multiple_of(t * TILE, TILE), TILE)
                x_rows[at, :] = x.astype(F32).T.astype(BF16)

    store = pltpu.make_async_copy(x_rows.at[pl.ds(0, rows)], out, row_sem)
    store.start()
    store.wait()


def body(
    points,
    counts,
    ln1_gain,
    ln1_bias,
    w_in,
    w_fx,
    w_slice,
    temper,
    query_weight,
    key_weight,
    value_weight,
    w_out,
    b_out,
    ln2_gain,
    ln2_bias,
    w_up,
    w_down,
):
    groups = lax.axis_size("head")
    shards = lax.axis_size("pts")
    rows = points.shape[0] // groups
    layers, width, part = w_in.shape
    assert part == DH
    hidden = w_up.shape[2]
    spread = groups * M
    tiles = -(-rows // TILE)
    vmem = pl.BlockSpec(memory_space=pltpu.VMEM)
    smem = pl.BlockSpec(memory_space=pltpu.SMEM)
    hbm = pl.BlockSpec(memory_space=pl.ANY)
    dma = pltpu.SemaphoreType.DMA
    return pl.pallas_call(
        functools.partial(kernel, groups, shards, rows, tiles),
        out_shape=jax.ShapeDtypeStruct((rows, width), BF16),
        in_specs=[smem, smem, hbm] + [vmem] * 14,
        out_specs=hbm,
        scratch_shapes=[
            pltpu.VMEM((tiles * TILE, width), BF16),
            pltpu.VMEM((tiles, width, TILE), BF16),
            pltpu.VMEM((tiles, width, TILE), BF16),
            pltpu.VMEM((tiles, spread, TILE), BF16),
            pltpu.VMEM((layers, spread, width), BF16),
            pltpu.VMEM((layers, hidden, width), BF16),
            pltpu.VMEM((layers, width, hidden), BF16),
            pltpu.VMEM((layers, spread, width), BF16),
            pltpu.VMEM((layers, spread, width), BF16),
            pltpu.VMEM((-(-5 * layers // 8) * 8, width), F32),
            pltpu.VMEM((5 * layers, width, TILE), F32),
            pltpu.VMEM((layers, spread, width + 128), F32),
            pltpu.VMEM((layers, 2, M, spread), BF16),
            pltpu.VMEM((layers, 2 * groups, M, spread), BF16),
            pltpu.VMEM((layers, M, spread), BF16),
            pltpu.VMEM((layers, shards, M, spread), BF16),
            pltpu.VMEM((2, M, spread), F32),
            pltpu.VMEM((3, spread, spread), F32),
            dma,
            dma((layers, groups)),
            dma((layers, groups)),
            dma((layers, 2 * groups)),
            dma((layers, 2 * groups)),
            dma((layers, shards)),
            dma((layers, shards)),
            dma((2, groups)),
            dma((2, groups)),
        ],
        compiler_params=pltpu.CompilerParams(collective_id=0, has_side_effects=True),
    )(
        counts,
        temper,
        points,
        ln1_gain,
        ln1_bias,
        w_in.swapaxes(1, 2),
        w_fx.swapaxes(1, 2),
        w_slice,
        query_weight,
        key_weight,
        value_weight,
        w_out,
        b_out,
        ln2_gain,
        ln2_bias,
        w_up,
        w_down,
    )


def solution(mesh):
    placed = (
        P("pts", None),
        P("pts"),
        P(),
        P(),
        P(None, None, "head"),
        P(None, None, "head"),
        P(),
        P(),
        P(),
        P(),
        P(),
        P(None, "head", None),
        P(),
        P(),
        P(),
        P(),
        P(),
    )
    return jax.shard_map(
        body, mesh=mesh, in_specs=placed, out_specs=P(("pts", "head"), None), check_vma=False
    )
```
